32 devices in a mesh: row: 2 (over x), col: 16 (over z, y, core).
Axes of the slice: x: 2, y: 2, z: 4, core: 2. Of those that a mesh axis runs over, the one named last changes fastest.
Arguments:
- panel: bfloat16 [49152, 1024], P('col', 'row'), may hold values from -0.1875 to 0.1875
- rhs: float32 [1024, 49152], P('row', 'col'), may hold values from -6 to 6
- diag_inverse: bfloat16 [2, 512, 512], replicated, may hold values from -1 to 2, as said below
Outputs:
- solved: bfloat16 [1024, 1024], P(None, 'row')
- updated: float32 [1024, 49152], P('row', 'col')
The draws below stay inside these ranges and needn't reach their ends.
Inputs may be any that keep to these rules, and one draw needn't show every extreme that they name: `diag_inverse`: each block is lower triangular; its diagonal entries are 0.5 or more.
All inputs are finite; a program needn't handle non-finite values.
Results may differ from the reference program's by a relative error of at most 0.0065.
Values may be sent and summed in bfloat16 or wider, within the bound.
A program may use at most 128 MiB of HBM per device.

```python
import jax
import jax.numpy as jnp
from jax import lax

NB = 512
NBR_DEV = 6
NRHS = 1024
STEPS = 2
N = 49152


def draw_diag_inverse(key, part):
    base = jax.random.fold_in(key, 11)
    first_key, second_key = jax.random.split(base)
    spread = jnp.clip(jax.random.normal(first_key, (STEPS, NB, NB), jnp.float32), -3.0, 3.0)
    diagonal = jax.random.uniform(second_key, (STEPS, NB), jnp.float32, 0.6, 1.6)
    lower = jnp.tril(spread, -1) / jnp.sqrt(jnp.float32(NB))
    whole = lower + jnp.eye(NB, dtype=jnp.float32)[None, :, :] * diagonal[:, :, None]
    return whole.astype(jnp.bfloat16)


def block_levels(stream_key, shape, cuts, smallest, top_value):
    def one(dim, blocks):
        steps = jax.random.uniform(jax.random.fold_in(jax.random.fold_in(stream_key, 6), dim), (blocks,), jnp.float32, smallest / len(cuts), top_value / len(cuts))
        return jnp.repeat(jnp.exp(steps), shape[dim] // blocks).reshape((-1,) + (1,) * (len(shape) - dim - 1))

    gain = one(*cuts[0])
    for cut in cuts[1:]:
        gain = gain * one(*cut)
    return gain


def bell_draw(stream_key, extent, scale, most, cuts=(), held_as=jnp.bfloat16):
    drawn = scale * jax.random.normal(stream_key, extent, jnp.float32)
    if cuts:
        drawn = drawn * block_levels(stream_key, extent, cuts, -0.22, 0.18)
    return jnp.clip(drawn, -most, most).astype(held_as)


def setup_inputs(seed: int = 0) -> dict:
    keys = jax.random.split(jax.random.key(seed), 4)
    panel = bell_draw(keys[0], (N, STEPS * NB), (STEPS * NB) ** -0.5, 0.1875, ((0, 16), (1, 2)))
    rhs = bell_draw(keys[1], (NRHS, N), 1.0, 6.0, ((0, 2), (1, 16)), jnp.float32)
    diag_inverse = draw_diag_inverse(jax.random.fold_in(keys[3], 71), 0)
    return dict(panel=panel, rhs=rhs, diag_inverse=diag_inverse)


def reference(panel, rhs, diag_inverse):
    rows_dev = NBR_DEV * NB
    masked = panel
    for current in range(STEPS):
        start = current * rows_dev
        masked = masked.at[start:start + NB, current * NB:].set(jnp.zeros((), jnp.bfloat16))
    pieces = []
    for current in range(STEPS):
        start = current * rows_dev
        residual = rhs[:, start:start + NB]
        if current > 0:
            earlier = jnp.concatenate(pieces, axis=1)
            factor_rows = masked[start:start + NB, 0:current * NB]
            products = lax.dot_general(earlier, factor_rows, (((1,), (1,)), ((), ())), preferred_element_type=jnp.float32)
            residual = residual - products
        inverse = diag_inverse[current].astype(jnp.float32)
        solution = jnp.dot(residual, inverse.T, precision=lax.Precision.HIGHEST)
        pieces.append(solution.astype(jnp.bfloat16))
    solved = jnp.concatenate(pieces, axis=1)
    window = lax.dot_general(solved, masked, (((1,), (1,)), ((), ())), preferred_element_type=jnp.float32)
    updated = rhs - window
    return solved, updated
```

```python
import functools

import jax
import jax.numpy as jnp
from jax import lax
from jax.experimental import pallas as pl
from jax.experimental.pallas import tpu as pltpu
from jax.sharding import PartitionSpec as P

PIECES = 4
MESH = pl.DeviceIdType.MESH
CONTRACT = (((1,), (1,)), ((), ()))


def times_transposed(left, right):
    return lax.dot_general(left, right, CONTRACT, preferred_element_type=jnp.float32)


def solve(residual, inverse):
    high = residual.astype(jnp.bfloat16)
    rest = residual - high.astype(jnp.float32)
    middle = rest.astype(jnp.bfloat16)
    low = (rest - middle.astype(jnp.float32)).astype(jnp.bfloat16)
    total = times_transposed(low, inverse) + times_transposed(middle, inverse)
    return (total + times_transposed(high, inverse)).astype(jnp.bfloat16)


def kernel(
    cols,
    panel_hbm,
    rhs_hbm,
    inverse_hbm,
    solved_ref,
    updated_ref,
    pan,
    quarter,
    inverse_ref,
    load_panel,
    load_rhs,
    load_inverse,
    panel_send,
    panel_recv,
    piece_send,
    piece_recv,
):
    steps, block = inverse_hbm.shape[0], inverse_hbm.shape[1]
    blocks = panel_hbm.shape[0] // block
    rows = block // PIECES
    chips = cols // 2
    i = lax.axis_index("row")
    c = lax.axis_index("col")
    other = 1 - i
    core = lax.rem(c, 2)
    chip = lax.div(c, 2)
    mate = c + 1 - 2 * core
    root = chip == 0
    is_first = core == 0
    has_child = chip + 2 < chips
    has_second = root & (chips > 1)

    def dropped(k):
        return (c < steps) & (k >= c)

    def rhs_load(j):
        at = pl.ds(pl.multiple_of(j * block, block), block)
        return pltpu.make_async_copy(rhs_hbm.at[:, at], updated_ref.at[:, at], load_rhs.at[j])

    def panel_load(j):
        at = pl.ds(pl.multiple_of(j * block, block), block)
        return pltpu.make_async_copy(panel_hbm.at[at, :], pan.at[i, at, :], load_panel.at[j])

    def panel_copy(j, which):
        at = pl.ds(pl.multiple_of(j * block, block), block)
        return pltpu.make_async_remote_copy(
            src_ref=pan.at[which, at, :],
            dst_ref=pan.at[which, at, :],
            send_sem=panel_send.at[j],
            recv_sem=panel_recv.at[j],
            device_id=(other, c),
            device_id_type=MESH,
        )

    def piece_copy(source, target, p, way, device):
        at = pl.ds(p * rows, rows)
        return pltpu.make_async_remote_copy(
            src_ref=quarter.at[source, at, :],
            dst_ref=quarter.at[target, at, :],
            send_sem=piece_send.at[way, source, p],
            recv_sem=piece_recv.at[target, p],
            device_id=device,
            device_id_type=MESH,
        )

    inverse_load = pltpu.make_async_copy(
        inverse_hbm.at[core], inverse_ref, load_inverse
    )
    rhs_load(0).start()
    inverse_load.start()

    @pl.when(jnp.logical_not(dropped(i)))
    def _():
        panel_load(0).start()

    for j in range(1, blocks):
        panel_load(j).start()
    for j in range(1, blocks):
        rhs_load(j).start()

    barrier = pltpu.get_barrier_semaphore()

    def greet(device):
        pl.semaphore_signal(barrier, inc=1, device_id=device, device_id_type=MESH)

    cross_pair = ((i == 0) & (c == 1)) | ((i == 1) & (c == 0))
    greet((other, c))
    greet((i, mate))

    @pl.when(has_child)
    def _():
        greet((i, c + 4))

    @pl.when(has_second)
    def _():
        greet((i, c + 2))

    @pl.when(chip == 1)
    def _():
        greet((i, c - 2))

    @pl.when(chip >= 2)
    def _():
        greet((i, c - 4))

    @pl.when(cross_pair)
    def _():
        greet((other, 1 - c))

    count = (
        2
        + has_child.astype(jnp.int32)
        + has_second.astype(jnp.int32)
        + (chip >= 1).astype(jnp.int32)
        + cross_pair.astype(jnp.int32)
    )
    pl.semaphore_wait(barrier, count)

    @pl.when(jnp.logical_not(dropped(i)))
    def _():
        panel_load(0).wait()
        panel_copy(0, i).start()

    for k in range(steps):

        @pl.when(dropped(k))
        def _(k=k):
            pan[k, pl.ds(0, block), :] = jnp.zeros((block, block), jnp.bfloat16)

    def send_rest():
        for j in range(1, blocks):
            panel_load(j).wait()
            panel_copy(j, i).start()

    pl.when(jnp.logical_not(root))(send_rest)
    inverse_load.wait()
    rhs_load(0).wait()

    def forward(slot, p):
        piece_copy(slot, slot, p, 0, (i, mate)).start()

        @pl.when(has_child)
        def _():
            piece_copy(slot, slot, p, 1, (i, c + 4)).start()

        @pl.when(has_second)
        def _():
            piece_copy(slot, slot, p, 2, (i, c + 2)).start()

    def forward_sent(slot, p):
        piece_copy(slot, slot, p, 0, (i, mate)).wait_send()

        @pl.when(has_child)
        def _():
            piece_copy(slot, slot, p, 1, (i, c + 4)).wait_send()

        @pl.when(has_second)
        def _():
            piece_copy(slot, slot, p, 2, (i, c + 2)).wait_send()

    def arrived(slot, p):
        piece_copy(slot, slot, p, 0, (i, mate)).wait_recv()

    @pl.when(is_first)
    def _():
        @pl.when(root)
        def _():
            quarter[0] = solve(updated_ref[:, pl.ds(0, block)], inverse_ref[...])
            for p in range(PIECES):

                @pl.when(i == 1)
                def _(p=p):
                    piece_copy(0, 2, p, 3, (other, c)).start()

                forward(0, p)
            send_rest()

        @pl.when(jnp.logical_not(root))
        def _():
            for p in range(PIECES):
                arrived(0, p)
                forward(0, p)

        for p in range(PIECES):
            arrived(2, p)
            forward(2, p)
        for p in range(PIECES):
            arrived(1, p)

    @pl.when(jnp.logical_not(is_first))
    def _():
        @pl.when(root)
        def _():
            for p in range(PIECES):
                arrived(0, p)

            @pl.when(i == 1)
            def _():
                panel_copy(0, other).wait_recv()

            residual = updated_ref[:, pl.ds(0, block)] - times_transposed(
                quarter[0], pan[0, pl.ds(0, block), :]
            )
            quarter[1] = solve(residual, inverse_ref[...])
            for p in range(PIECES):

                @pl.when(i == 0)
                def _(p=p):
                    piece_copy(1, 2, p, 3, (other, 1 - c)).start()

                forward(1, p)
            send_rest()

        @pl.when(jnp.logical_not(root))
        def _():
            for p in range(PIECES):
                arrived(1, p)
                forward(1, p)
            for p in range(PIECES):
                arrived(0, p)

        for p in range(PIECES):
            arrived(2, p)

    solved_ref[pl.ds(pl.multiple_of(i * block, block), block), :] = quarter[i]
    solved_ref[pl.ds(pl.multiple_of(other * block, block), block), :] = quarter[2]

    early = (c == 1) & (i == 1)

    @pl.when(jnp.logical_not(dropped(other)) & jnp.logical_not(early))
    def _():
        panel_copy(0, other).wait_recv()

    def update(j):
        at = pl.ds(pl.multiple_of(j * block, block), block)
        total = times_transposed(quarter[0], pan[0, at, :])
        total = total + times_transposed(quarter[1], pan[1, at, :])
        updated_ref[:, at] = updated_ref[:, at] - total

    update(0)

    def chunk(j, carry):
        rhs_load(j).wait()
        panel_copy(j, other).wait_recv()
        update(j)
        return carry

    lax.fori_loop(1, blocks, chunk, 0)

    @pl.when(jnp.logical_not(dropped(i)))
    def _():
        panel_copy(0, i).wait_send()

    for j in range(1, blocks):
        panel_copy(j, i).wait_send()
    for p in range(PIECES):

        @pl.when(is_first)
        def _(p=p):
            forward_sent(0, p)
            forward_sent(2, p)

            @pl.when(root & (i == 1))
            def _():
                piece_copy(0, 2, p, 3, (other, c)).wait_send()

        @pl.when(jnp.logical_not(is_first))
        def _(p=p):
            forward_sent(1, p)

            @pl.when(root & (i == 0))
            def _():
                piece_copy(1, 2, p, 3, (other, 1 - c)).wait_send()


def shards(panel, rhs, diag_inverse):
    steps, block = diag_inverse.shape[:2]
    blocks = panel.shape[0] // block
    return pl.pallas_call(
        functools.partial(kernel, lax.axis_size("col")),
        out_shape=(
            pltpu.VMEM((steps * block, block), jnp.bfloat16),
            pltpu.VMEM(rhs.shape, jnp.float32),
        ),
        in_specs=[pl.BlockSpec(memory_space=pltpu.HBM)] * 3,
        out_specs=(pl.BlockSpec(memory_space=pltpu.VMEM),) * 2,
        scratch_shapes=[
            pltpu.VMEM((steps,) + panel.shape, jnp.bfloat16),
            pltpu.VMEM((3, block, block), jnp.bfloat16),
            pltpu.VMEM((block, block), jnp.bfloat16),
            pltpu.SemaphoreType.DMA((blocks,)),
            pltpu.SemaphoreType.DMA((blocks,)),
            pltpu.SemaphoreType.DMA,
            pltpu.SemaphoreType.DMA((blocks,)),
            pltpu.SemaphoreType.DMA((blocks,)),
            pltpu.SemaphoreType.DMA((4, 3, PIECES)),
            pltpu.SemaphoreType.DMA((3, PIECES)),
        ],
        compiler_params=pltpu.CompilerParams(
            collective_id=0, has_side_effects=True, vmem_limit_bytes=56 * 1024 * 1024
        ),
    )(panel, rhs, diag_inverse)


def solution(mesh):
    placed = (P("col", "row"), P("row", "col"), P())
    return jax.shard_map(
        shards,
        mesh=mesh,
        in_specs=placed,
        out_specs=(P(None, "row"), P("row", "col")),
        check_vma=False,
    )
```

```python
import functools

import jax
import jax.numpy as jnp
from jax import lax
from jax.experimental import pallas as pl
from jax.experimental.pallas import tpu as pltpu
from jax.sharding import PartitionSpec as P

PIECES = 4
MESH = pl.DeviceIdType.MESH
CONTRACT = (((1,), (1,)), ((), ()))


def times_transposed(left, right):
    return lax.dot_general(left, right, CONTRACT, preferred_element_type=jnp.float32)


def solve(residual, inverse):
    high = residual.astype(jnp.bfloat16)
    rest = residual - high.astype(jnp.float32)
    middle = rest.astype(jnp.bfloat16)
    low = (rest - middle.astype(jnp.float32)).astype(jnp.bfloat16)
    total = times_transposed(low, inverse) + times_transposed(middle, inverse)
    return (total + times_transposed(high, inverse)).astype(jnp.bfloat16)


def kernel(
    cols,
    panel_hbm,
    rhs_hbm,
    inverse_hbm,
    updated_ref,
    pan,
    quarter,
    inverse_ref,
    load_panel,
    load_rhs,
    load_inverse,
    panel_send,
    panel_recv,
    piece_send,
    piece_recv,
):
    steps, block = inverse_hbm.shape[0], inverse_hbm.shape[1]
    blocks = panel_hbm.shape[0] // block
    rows = block // PIECES
    chips = cols // 2
    i = lax.axis_index("row")
    c = lax.axis_index("col")
    other = 1 - i
    core = lax.rem(c, 2)
    chip = lax.div(c, 2)
    mate = c + 1 - 2 * core
    root = chip == 0
    is_first = core == 0
    has_child = chip + 2 < chips
    has_second = root & (chips > 1)

    def dropped(k):
        return (c < steps) & (k >= c)

    def rhs_load(j):
        at = pl.ds(pl.multiple_of(j * block, block), block)
        return pltpu.make_async_copy(rhs_hbm.at[:, at], updated_ref.at[:, at], load_rhs.at[j])

    def panel_load(j):
        at = pl.ds(pl.multiple_of(j * block, block), block)
        return pltpu.make_async_copy(panel_hbm.at[at, :], pan.at[i, at, :], load_panel.at[j])

    def panel_copy(j, which):
        at = pl.ds(pl.multiple_of(j * block, block), block)
        return pltpu.make_async_remote_copy(
            src_ref=pan.at[which, at, :],
            dst_ref=pan.at[which, at, :],
            send_sem=panel_send.at[j],
            recv_sem=panel_recv.at[j],
            device_id=(other, c),
            device_id_type=MESH,
        )

    def piece_copy(source, target, p, way, device):
        at = pl.ds(p * rows, rows)
        return pltpu.make_async_remote_copy(
            src_ref=quarter.at[source, at, :],
            dst_ref=quarter.at[target, at, :],
            send_sem=piece_send.at[way, source, p],
            recv_sem=piece_recv.at[target, p],
            device_id=device,
            device_id_type=MESH,
        )

    barrier = pltpu.get_barrier_semaphore()

    def greet(device):
        pl.semaphore_signal(barrier, inc=1, device_id=device, device_id_type=MESH)

    cross_pair = ((i == 0) & (c == 1)) | ((i == 1) & (c == 0))
    greet((other, c))
    greet((i, mate))

    @pl.when(has_child)
    def _():
        greet((i, c + 4))

    @pl.when(has_second)
    def _():
        greet((i, c + 2))

    @pl.when(chip == 1)
    def _():
        greet((i, c - 2))

    @pl.when(chip >= 2)
    def _():
        greet((i, c - 4))

    @pl.when(cross_pair)
    def _():
        greet((other, 1 - c))

    inverse_load = pltpu.make_async_copy(
        inverse_hbm.at[core], inverse_ref, load_inverse
    )
    rhs_load(0).start()
    inverse_load.start()

    @pl.when(jnp.logical_not(dropped(i)))
    def _():
        panel_load(0).start()

    for j in range(1, blocks):
        panel_load(j).start()
    for j in range(1, blocks):
        rhs_load(j).start()

    count = (
        2
        + has_child.astype(jnp.int32)
        + has_second.astype(jnp.int32)
        + (chip >= 1).astype(jnp.int32)
        + cross_pair.astype(jnp.int32)
    )
    pl.semaphore_wait(barrier, count)

    @pl.when(jnp.logical_not(dropped(i)))
    def _():
        panel_load(0).wait()
        panel_copy(0, i).start()

    for k in range(steps):

        @pl.when(dropped(k))
        def _(k=k):
            pan[k, pl.ds(0, block), :] = jnp.zeros((block, block), jnp.bfloat16)

    def send_rest():
        for j in range(1, blocks):
            panel_load(j).wait()
            panel_copy(j, i).start()

    pl.when(jnp.logical_not(root))(send_rest)
    inverse_load.wait()
    rhs_load(0).wait()

    def forward(slot, p):
        piece_copy(slot, slot, p, 0, (i, mate)).start()

        @pl.when(has_child)
        def _():
            piece_copy(slot, slot, p, 1, (i, c + 4)).start()

        @pl.when(has_second)
        def _():
            piece_copy(slot, slot, p, 2, (i, c + 2)).start()

    def forward_sent(slot, p):
        piece_copy(slot, slot, p, 0, (i, mate)).wait_send()

        @pl.when(has_child)
        def _():
            piece_copy(slot, slot, p, 1, (i, c + 4)).wait_send()

        @pl.when(has_second)
        def _():
            piece_copy(slot, slot, p, 2, (i, c + 2)).wait_send()

    def arrived(slot, p):
        piece_copy(slot, slot, p, 0, (i, mate)).wait_recv()

    @pl.when(is_first)
    def _():
        @pl.when(root)
        def _():
            quarter[0] = solve(updated_ref[:, pl.ds(0, block)], inverse_ref[...])
            for p in range(PIECES):

                @pl.when(i == 1)
                def _(p=p):
                    piece_copy(0, 2, p, 3, (other, c)).start()

                forward(0, p)
            send_rest()

        @pl.when(jnp.logical_not(root))
        def _():
            for p in range(PIECES):
                arrived(0, p)
                forward(0, p)

        for p in range(PIECES):
            arrived(2, p)
            forward(2, p)
        for p in range(PIECES):
            arrived(1, p)

    @pl.when(jnp.logical_not(is_first))
    def _():
        @pl.when(root)
        def _():
            for p in range(PIECES):
                arrived(0, p)

            @pl.when(i == 1)
            def _():
                panel_copy(0, other).wait_recv()

            residual = updated_ref[:, pl.ds(0, block)] - times_transposed(
                quarter[0], pan[0, pl.ds(0, block), :]
            )
            quarter[1] = solve(residual, inverse_ref[...])
            for p in range(PIECES):

                @pl.when(i == 0)
                def _(p=p):
                    piece_copy(1, 2, p, 3, (other, 1 - c)).start()

                forward(1, p)
            send_rest()

        @pl.when(jnp.logical_not(root))
        def _():
            for p in range(PIECES):
                arrived(1, p)
                forward(1, p)
            for p in range(PIECES):
                arrived(0, p)

        for p in range(PIECES):
            arrived(2, p)

    early = (c == 1) & (i == 1)

    @pl.when(jnp.logical_not(dropped(other)) & jnp.logical_not(early))
    def _():
        panel_copy(0, other).wait_recv()

    def update(j):
        at = pl.ds(pl.multiple_of(j * block, block), block)
        total = times_transposed(quarter[0], pan[0, at, :])
        total = total + times_transposed(quarter[1], pan[1, at, :])
        updated_ref[:, at] = updated_ref[:, at] - total

    update(0)

    def chunk(j, carry):
        rhs_load(j).wait()
        panel_copy(j, other).wait_recv()
        update(j)
        return carry

    lax.fori_loop(1, blocks - 1, chunk, 0)
    rhs_load(blocks - 1).wait()
    panel_copy(blocks - 1, other).wait_recv()

    @pl.when(jnp.logical_not(dropped(i)))
    def _():
        panel_copy(0, i).wait_send()

    for j in range(1, blocks):
        panel_copy(j, i).wait_send()
    for p in range(PIECES):

        @pl.when(is_first)
        def _(p=p):
            forward_sent(0, p)
            forward_sent(2, p)

            @pl.when(root & (i == 1))
            def _():
                piece_copy(0, 2, p, 3, (other, c)).wait_send()

        @pl.when(jnp.logical_not(is_first))
        def _(p=p):
            forward_sent(1, p)

            @pl.when(root & (i == 0))
            def _():
                piece_copy(1, 2, p, 3, (other, 1 - c)).wait_send()


def writer(updated_ref, pan, quarter, solved_hbm, updated_hbm, last, done_sem, last_sem, solved_sem):
    block = quarter.shape[1]
    blocks = updated_ref.shape[1] // block
    i = lax.axis_index("row")
    copies = []

    def put(j):
        at = pl.ds(j * block, block)
        copies.append(
            pltpu.make_async_copy(updated_ref.at[:, at], updated_hbm.at[:, at], done_sem.at[j])
        )
        copies[-1].start()

    for j in range(blocks - 1):
        put(j)
    for part, slot in enumerate((i, 2)):
        half = i if part == 0 else 1 - i
        at = pl.ds(pl.multiple_of(half * block, block), block)
        copies.append(
            pltpu.make_async_copy(quarter.at[slot], solved_hbm.at[at, :], solved_sem.at[part])
        )
        copies[-1].start()
    width = block // 2
    for part in range(2):
        start = (blocks - 1) * block + part * width
        at = pl.ds(start, width)
        total = times_transposed(quarter[0], pan[0, at, :])
        total = total + times_transposed(quarter[1], pan[1, at, :])
        last[part] = updated_ref[:, at] - total
        copies.append(
            pltpu.make_async_copy(last.at[part], updated_hbm.at[:, at], last_sem.at[part])
        )
        copies[-1].start()
    for copy in copies:
        copy.wait()


def shards(panel, rhs, diag_inverse):
    steps, block = diag_inverse.shape[:2]
    blocks = panel.shape[0] // block
    parts = pl.pallas_call(
        functools.partial(kernel, lax.axis_size("col")),
        out_shape=(
            pltpu.VMEM(rhs.shape, jnp.float32),
            pltpu.VMEM((steps,) + panel.shape, jnp.bfloat16),
            pltpu.VMEM((3, block, block), jnp.bfloat16),
        ),
        in_specs=[pl.BlockSpec(memory_space=pltpu.HBM)] * 3,
        out_specs=(pl.BlockSpec(memory_space=pltpu.VMEM),) * 3,
        scratch_shapes=[
            pltpu.VMEM((block, block), jnp.bfloat16),
            pltpu.SemaphoreType.DMA((blocks,)),
            pltpu.SemaphoreType.DMA((blocks,)),
            pltpu.SemaphoreType.DMA,
            pltpu.SemaphoreType.DMA((blocks,)),
            pltpu.SemaphoreType.DMA((blocks,)),
            pltpu.SemaphoreType.DMA((4, 3, PIECES)),
            pltpu.SemaphoreType.DMA((3, PIECES)),
        ],
        compiler_params=pltpu.CompilerParams(
            collective_id=0, has_side_effects=True, vmem_limit_bytes=49 * 1024 * 1024
        ),
    )(panel, rhs, diag_inverse)
    return pl.pallas_call(
        writer,
        out_shape=(
            jax.ShapeDtypeStruct((steps * block, block), jnp.bfloat16),
            jax.ShapeDtypeStruct(rhs.shape, jnp.float32),
        ),
        in_specs=[pl.BlockSpec(memory_space=pltpu.VMEM)] * 3,
        out_specs=(pl.BlockSpec(memory_space=pltpu.HBM),) * 2,
        scratch_shapes=[
            pltpu.VMEM((2, rhs.shape[0], block // 2), jnp.float32),
            pltpu.SemaphoreType.DMA((blocks,)),
            pltpu.SemaphoreType.DMA((2,)),
            pltpu.SemaphoreType.DMA((2,)),
        ],
        compiler_params=pltpu.CompilerParams(vmem_limit_bytes=16 * 1024 * 1024),
    )(*parts)


def solution(mesh):
    placed = (P("col", "row"), P("row", "col"), P())
    return jax.shard_map(
        shards,
        mesh=mesh,
        in_specs=placed,
        out_specs=(P(None, "row"), P("row", "col")),
        check_vma=False,
    )
```

```python
import functools

import jax
import jax.numpy as jnp
from jax import lax
from jax.experimental import pallas as pl
from jax.experimental.pallas import tpu as pltpu
from jax.sharding import PartitionSpec as P

PIECES = 4
MESH = pl.DeviceIdType.MESH
CONTRACT = (((1,), (1,)), ((), ()))


def times_transposed(left, right):
    return lax.dot_general(left, right, CONTRACT, preferred_element_type=jnp.float32)


def cuts(blocks):
    return blocks // 2, blocks - 1


def only(condition):
    return (lambda f: f()) if condition is None else pl.when(condition)


def solve(residual, inverse):
    high = residual.astype(jnp.bfloat16)
    rest = residual - high.astype(jnp.float32)
    middle = rest.astype(jnp.bfloat16)
    low = (rest - middle.astype(jnp.float32)).astype(jnp.bfloat16)
    total = times_transposed(low, inverse) + times_transposed(middle, inverse)
    return (total + times_transposed(high, inverse)).astype(jnp.bfloat16)


def kernel(
    cols,
    panel_hbm,
    rhs_hbm,
    inverse_hbm,
    updated_ref,
    quarter,
    pan,
    inverse_ref,
    load_panel,
    load_rhs,
    load_inverse,
    panel_send,
    panel_recv,
    piece_send,
    piece_recv,
):
    steps, block = inverse_hbm.shape[0], inverse_hbm.shape[1]
    blocks = panel_hbm.shape[0] // block
    even_cut, odd_cut = cuts(blocks)
    rows = block // PIECES
    chips = cols // 2
    i = lax.axis_index("row")
    c = lax.axis_index("col")
    other = 1 - i
    core = lax.rem(c, 2)
    chip = lax.div(c, 2)
    mate = c + 1 - 2 * core
    root = chip == 0
    is_first = core == 0
    has_child = chip + 2 < chips
    has_second = root & (chips > 1)

    def mine(j):
        return None if j < even_cut else core == 1

    def dropped(k):
        return (c < steps) & (k >= c)

    def rhs_load(j):
        at = pl.ds(pl.multiple_of(j * block, block), block)
        return pltpu.make_async_copy(rhs_hbm.at[:, at], updated_ref.at[:, at], load_rhs.at[j])

    def panel_load(j):
        at = pl.ds(pl.multiple_of(j * block, block), block)
        return pltpu.make_async_copy(panel_hbm.at[at, :], pan.at[i, at, :], load_panel.at[j])

    def panel_copy(j, which):
        at = pl.ds(pl.multiple_of(j * block, block), block)
        return pltpu.make_async_remote_copy(
            src_ref=pan.at[which, at, :],
            dst_ref=pan.at[which, at, :],
            send_sem=panel_send.at[j],
            recv_sem=panel_recv.at[j],
            device_id=(other, c),
            device_id_type=MESH,
        )

    def piece_copy(source, target, p, way, device):
        at = pl.ds(p * rows, rows)
        return pltpu.make_async_remote_copy(
            src_ref=quarter.at[source, at, :],
            dst_ref=quarter.at[target, at, :],
            send_sem=piece_send.at[way, source, p],
            recv_sem=piece_recv.at[target, p],
            device_id=device,
            device_id_type=MESH,
        )

    barrier = pltpu.get_barrier_semaphore()

    def greet(device):
        pl.semaphore_signal(barrier, inc=1, device_id=device, device_id_type=MESH)

    cross_pair = ((i == 0) & (c == 1)) | ((i == 1) & (c == 0))
    greet((other, c))
    greet((i, mate))

    @pl.when(has_child)
    def _():
        greet((i, c + 4))

    @pl.when(has_second)
    def _():
        greet((i, c + 2))

    @pl.when(chip == 1)
    def _():
        greet((i, c - 2))

    @pl.when(chip >= 2)
    def _():
        greet((i, c - 4))

    @pl.when(cross_pair)
    def _():
        greet((other, 1 - c))

    inverse_load = pltpu.make_async_copy(
        inverse_hbm.at[core], inverse_ref, load_inverse
    )
    rhs_load(0).start()
    inverse_load.start()

    @pl.when(jnp.logical_not(dropped(i)))
    def _():
        panel_load(0).start()

    for j in range(1, odd_cut):

        @only(mine(j))
        def _(j=j):
            panel_load(j).start()
            rhs_load(j).start()

    count = (
        2
        + has_child.astype(jnp.int32)
        + has_second.astype(jnp.int32)
        + (chip >= 1).astype(jnp.int32)
        + cross_pair.astype(jnp.int32)
    )
    pl.semaphore_wait(barrier, count)

    @pl.when(jnp.logical_not(dropped(i)))
    def _():
        panel_load(0).wait()
        panel_copy(0, i).start()

    for k in range(steps):

        @pl.when(dropped(k))
        def _(k=k):
            pan[k, pl.ds(0, block), :] = jnp.zeros((block, block), jnp.bfloat16)

    def send_rest():
        for j in range(1, odd_cut):

            @only(mine(j))
            def _(j=j):
                panel_load(j).wait()
                panel_copy(j, i).start()

    pl.when(jnp.logical_not(root))(send_rest)
    inverse_load.wait()
    rhs_load(0).wait()

    def forward(slot, p):
        piece_copy(slot, slot, p, 0, (i, mate)).start()

        @pl.when(has_child)
        def _():
            piece_copy(slot, slot, p, 1, (i, c + 4)).start()

        @pl.when(has_second)
        def _():
            piece_copy(slot, slot, p, 2, (i, c + 2)).start()

    def forward_sent(slot, p):
        piece_copy(slot, slot, p, 0, (i, mate)).wait_send()

        @pl.when(has_child)
        def _():
            piece_copy(slot, slot, p, 1, (i, c + 4)).wait_send()

        @pl.when(has_second)
        def _():
            piece_copy(slot, slot, p, 2, (i, c + 2)).wait_send()

    def arrived(slot, p):
        piece_copy(slot, slot, p, 0, (i, mate)).wait_recv()

    @pl.when(is_first)
    def _():
        @pl.when(root)
        def _():
            quarter[0] = solve(updated_ref[:, pl.ds(0, block)], inverse_ref[...])
            for p in range(PIECES):

                @pl.when(i == 1)
                def _(p=p):
                    piece_copy(0, 2, p, 3, (other, c)).start()

                forward(0, p)
            send_rest()

        @pl.when(jnp.logical_not(root))
        def _():
            for p in range(PIECES):
                arrived(0, p)
                forward(0, p)

        for p in range(PIECES):
            arrived(2, p)
            forward(2, p)
        for p in range(PIECES):
            arrived(1, p)

    @pl.when(jnp.logical_not(is_first))
    def _():
        @pl.when(root)
        def _():
            for p in range(PIECES):
                arrived(0, p)

            @pl.when(i == 1)
            def _():
                panel_copy(0, other).wait_recv()

            residual = updated_ref[:, pl.ds(0, block)] - times_transposed(
                quarter[0], pan[0, pl.ds(0, block), :]
            )
            quarter[1] = solve(residual, inverse_ref[...])
            for p in range(PIECES):

                @pl.when(i == 0)
                def _(p=p):
                    piece_copy(1, 2, p, 3, (other, 1 - c)).start()

                forward(1, p)
            send_rest()

        @pl.when(jnp.logical_not(root))
        def _():
            for p in range(PIECES):
                arrived(1, p)
                forward(1, p)
            for p in range(PIECES):
                arrived(0, p)

        for p in range(PIECES):
            arrived(2, p)

    early = (c == 1) & (i == 1)

    @pl.when(jnp.logical_not(dropped(other)) & jnp.logical_not(early))
    def _():
        panel_copy(0, other).wait_recv()

    def update(j):
        at = pl.ds(pl.multiple_of(j * block, block), block)
        total = times_transposed(quarter[0], pan[0, at, :])
        total = total + times_transposed(quarter[1], pan[1, at, :])
        updated_ref[:, at] = updated_ref[:, at] - total

    update(0)

    def chunk(j, carry):
        rhs_load(j).wait()
        panel_copy(j, other).wait_recv()
        update(j)
        return carry

    lax.fori_loop(1, jnp.where(core == 1, odd_cut, even_cut), chunk, 0)

    @pl.when(jnp.logical_not(dropped(i)))
    def _():
        panel_copy(0, i).wait_send()

    for j in range(1, odd_cut):

        @only(mine(j))
        def _(j=j):
            panel_copy(j, i).wait_send()

    for p in range(PIECES):

        @pl.when(is_first)
        def _(p=p):
            forward_sent(0, p)
            forward_sent(2, p)

            @pl.when(root & (i == 1))
            def _():
                piece_copy(0, 2, p, 3, (other, c)).wait_send()

        @pl.when(jnp.logical_not(is_first))
        def _(p=p):
            forward_sent(1, p)

            @pl.when(root & (i == 0))
            def _():
                piece_copy(1, 2, p, 3, (other, 1 - c)).wait_send()


def first_writer(blocks, updated_ref, quarter, solved_hbm, updated_hbm, done_sem, solved_sem):
    block = quarter.shape[1]
    even_cut, odd_cut = cuts(blocks)
    i = lax.axis_index("row")
    core = lax.rem(lax.axis_index("col"), 2)

    def block_put(j):
        at = pl.ds(j * block, block)
        return pltpu.make_async_copy(updated_ref.at[:, at], updated_hbm.at[:, at], done_sem.at[j])

    def solved_put(part):
        slot, half = ((i, i), (2, 1 - i))[part]
        at = pl.ds(pl.multiple_of(half * block, block), block)
        return pltpu.make_async_copy(
            quarter.at[slot], solved_hbm.at[at, :], solved_sem.at[part]
        )

    for step in ("start", "wait"):
        for j in range(odd_cut):

            @only(None if j < even_cut else core == 1)
            def _(j=j, step=step):
                getattr(block_put(j), step)()

        for part in range(2):
            getattr(solved_put(part), step)()


def second_kernel(
    panel_hbm,
    rhs_hbm,
    quarter,
    solved_hbm,
    updated_ref,
    pan,
    kept,
    load_panel,
    load_rhs,
    panel_send,
    panel_recv,
):
    block = quarter.shape[1]
    blocks = panel_hbm.shape[0] // block
    even_cut, odd_cut = cuts(blocks)
    i = lax.axis_index("row")
    c = lax.axis_index("col")
    other = 1 - i
    core = lax.rem(c, 2)

    def mine(j):
        return None if j >= odd_cut else core == 0

    def rhs_load(j):
        return pltpu.make_async_copy(
            rhs_hbm.at[:, pl.ds(j * block, block)],
            updated_ref.at[:, pl.ds((j - even_cut) * block, block)],
            load_rhs.at[j - even_cut],
        )

    def panel_load(j):
        return pltpu.make_async_copy(
            panel_hbm.at[pl.ds(j * block, block), :],
            pan.at[i, pl.ds((j - even_cut) * block, block), :],
            load_panel.at[j - even_cut],
        )

    def panel_copy(j, which):
        at = pl.ds((j - even_cut) * block, block)
        return pltpu.make_async_remote_copy(
            src_ref=pan.at[which, at, :],
            dst_ref=pan.at[which, at, :],
            send_sem=panel_send.at[j - even_cut],
            recv_sem=panel_recv.at[j - even_cut],
            device_id=(other, c),
            device_id_type=MESH,
        )

    barrier = pltpu.get_barrier_semaphore()
    pl.semaphore_signal(barrier, inc=1, device_id=(other, c), device_id_type=MESH)
    for load in (panel_load, rhs_load):
        for j in range(even_cut, blocks):

            @only(mine(j))
            def _(j=j, load=load):
                load(j).start()

    pl.semaphore_wait(barrier, 1)
    for j in range(even_cut, blocks):

        @only(mine(j))
        def _(j=j):
            panel_load(j).wait()
            panel_copy(j, i).start()

    kept[...] = quarter[pl.ds(0, 2)]
    for j in range(even_cut, blocks):

        @only(mine(j))
        def _(j=j):
            rhs_load(j).wait()
            panel_copy(j, other).wait_recv()
            if j < blocks - 1:
                at = pl.ds((j - even_cut) * block, block)
                total = times_transposed(quarter[0], pan[0, at, :])
                total = total + times_transposed(quarter[1], pan[1, at, :])
                updated_ref[:, at] = updated_ref[:, at] - total

    for j in range(even_cut, blocks):

        @only(mine(j))
        def _(j=j):
            panel_copy(j, i).wait_send()


def second_writer(blocks, updated_ref, pan, quarter, _, updated_hbm, last, done_sem, last_sem):
    block = quarter.shape[1]
    even_cut, odd_cut = cuts(blocks)
    core = lax.rem(lax.axis_index("col"), 2)

    def block_put(j):
        return pltpu.make_async_copy(
            updated_ref.at[:, pl.ds((j - even_cut) * block, block)],
            updated_hbm.at[:, pl.ds(j * block, block)],
            done_sem.at[j - even_cut],
        )

    for j in range(even_cut, odd_cut):

        @pl.when(core == 0)
        def _(j=j):
            block_put(j).start()

    width = block // 2
    copies = []
    for part in range(2):
        start = (blocks - 1 - even_cut) * block + part * width
        at = pl.ds(start, width)
        total = times_transposed(quarter[0], pan[0, at, :])
        total = total + times_transposed(quarter[1], pan[1, at, :])
        last[part] = updated_ref[:, at] - total
        to = pl.ds(start + even_cut * block, width)
        copies.append(
            pltpu.make_async_copy(last.at[part], updated_hbm.at[:, to], last_sem.at[part])
        )
        copies[-1].start()
    for j in range(even_cut, odd_cut):

        @pl.when(core == 0)
        def _(j=j):
            block_put(j).wait()

    for copy in copies:
        copy.wait()


def shards(panel, rhs, diag_inverse):
    steps, block = diag_inverse.shape[:2]
    blocks = panel.shape[0] // block
    even_cut, odd_cut = cuts(blocks)
    rest = blocks - even_cut
    hbm = pl.BlockSpec(memory_space=pltpu.HBM)
    vmem = pl.BlockSpec(memory_space=pltpu.VMEM)
    dma = pltpu.SemaphoreType.DMA
    first, quarter = pl.pallas_call(
        functools.partial(kernel, lax.axis_size("col")),
        out_shape=(
            pltpu.VMEM((rhs.shape[0], odd_cut * block), jnp.float32),
            pltpu.VMEM((3, block, block), jnp.bfloat16),
        ),
        in_specs=[hbm] * 3,
        out_specs=(vmem,) * 2,
        scratch_shapes=[
            pltpu.VMEM((steps, odd_cut * block, block), jnp.bfloat16),
            pltpu.VMEM((block, block), jnp.bfloat16),
            dma((blocks,)),
            dma((blocks,)),
            dma,
            dma((blocks,)),
            dma((blocks,)),
            dma((4, 3, PIECES)),
            dma((3, PIECES)),
        ],
        compiler_params=pltpu.CompilerParams(
            collective_id=0, has_side_effects=True, vmem_limit_bytes=57 * 1024 * 1024
        ),
    )(panel, rhs, diag_inverse)
    solved, updated = pl.pallas_call(
        functools.partial(first_writer, blocks),
        out_shape=(
            jax.ShapeDtypeStruct((steps * block, block), jnp.bfloat16),
            jax.ShapeDtypeStruct(rhs.shape, jnp.float32),
        ),
        in_specs=[vmem] * 2,
        out_specs=(hbm,) * 2,
        scratch_shapes=[dma((blocks,)), dma((2,))],
        compiler_params=pltpu.CompilerParams(vmem_limit_bytes=16 * 1024 * 1024),
    )(first, quarter)
    second, pan, kept = pl.pallas_call(
        second_kernel,
        out_shape=(
            pltpu.VMEM((rhs.shape[0], rest * block), jnp.float32),
            pltpu.VMEM((steps, rest * block, block), jnp.bfloat16),
            pltpu.VMEM((2, block, block), jnp.bfloat16),
        ),
        in_specs=[hbm, hbm, vmem, hbm],
        out_specs=(vmem,) * 3,
        scratch_shapes=[dma((rest,)), dma((rest,)), dma((rest,)), dma((rest,))],
        compiler_params=pltpu.CompilerParams(
            collective_id=1, has_side_effects=True, vmem_limit_bytes=54 * 1024 * 1024
        ),
    )(panel, rhs, quarter, solved)
    updated = pl.pallas_call(
        functools.partial(second_writer, blocks),
        out_shape=jax.ShapeDtypeStruct(rhs.shape, jnp.float32),
        in_specs=[vmem] * 3 + [hbm],
        out_specs=hbm,
        scratch_shapes=[
            pltpu.VMEM((2, rhs.shape[0], block // 2), jnp.float32),
            dma((rest,)),
            dma((2,)),
        ],
        input_output_aliases={3: 0},
        compiler_params=pltpu.CompilerParams(vmem_limit_bytes=16 * 1024 * 1024),
    )(second, pan, kept, updated)
    return solved, updated


def solution(mesh):
    placed = (P("col", "row"), P("row", "col"), P())
    return jax.shard_map(
        shards,
        mesh=mesh,
        in_specs=placed,
        out_specs=(P(None, "row"), P("row", "col")),
        check_vma=False,
    )
```
